256 devices in a mesh: group: 8 (over z), shard: 32 (over x, y, core).
Axes of the slice: x: 4, y: 4, z: 8, core: 2. Of those that a mesh axis runs over, the one named last changes fastest.
Arguments:
- queries: bfloat16 [1536, 1024], P(('group', 'shard')), may hold values from -12 to 12
- candidates: bfloat16 [1048576, 1024], P(('group', 'shard')), may hold values from -4 to 4
- targets: int32 [1536], replicated, may hold values from 0 to 1048575
Outputs:
- losses: float32 [1536], replicated
- mean_loss: float32 [], replicated
The draws below stay inside these ranges and needn't reach their ends.
All inputs are finite; a program needn't handle non-finite values.
Results may differ from the reference program's by a relative error of at most 0.0003.
Values may be sent and summed in bfloat16 or wider, within the bound.
A program may use at most 64 MiB of HBM per device.

```python
import jax
import jax.numpy as jnp
from jax import lax

D = 1024
CAND_DEV = 4096
QUERIES = 1536
CANDS = 1048576
N_GROUP = 8
N_SHARD = 32


def shared_queries(key):
    normal_key = jax.random.fold_in(key, 11)
    base = jnp.clip(jax.random.normal(normal_key, (QUERIES, D), jnp.float32), -6.0, 6.0)
    return base


def draw_queries(key, part):
    base = shared_queries(key)
    return base.astype(jnp.bfloat16)


def draw_candidates(key, part):
    cand_key = jax.random.fold_in(key, 21)
    size_key = jax.random.fold_in(key, 22)
    order_key = jax.random.fold_in(key, 31)
    offset_key = jax.random.fold_in(key, 32)
    height_key = jax.random.fold_in(key, 33)
    row_sizes = 0.5 * jnp.exp(jax.random.uniform(size_key, (CANDS, 1), jnp.float32, 0.0, 1.0) * jnp.log(8.0))
    rows = jnp.clip(jax.random.normal(cand_key, (CANDS, D), jnp.float32), -6.0, 6.0)
    rows = rows * row_sizes * D ** (-0.5)
    base = shared_queries(key)
    plant_norms = 0.5 * jnp.exp(jax.random.uniform(height_key, (QUERIES,), jnp.float32, 0.0, 1.0) * jnp.log(8.0))
    heights = plant_norms * D ** (-0.5)
    strong = jnp.arange(QUERIES, dtype=jnp.int32) < 8
    heights = jnp.where(strong, jnp.float32(min(4.0, 300.0 / D)), heights)
    aligned = jnp.where(base >= 0.0, heights[:, None], -heights[:, None])
    stride = CANDS // QUERIES
    order = jax.random.permutation(order_key, QUERIES).astype(jnp.int32)
    offsets = jax.random.randint(offset_key, (QUERIES,), 0, stride, jnp.int32)
    places = order * stride + offsets
    rows = rows.at[places].set(aligned)
    return rows.astype(jnp.bfloat16)


def plant(values, own_key, least, top_value):
    index_at = [jax.random.randint(jax.random.fold_in(own_key, axis), (), 0, length) for axis, length in enumerate(values.shape)]
    widest = values.shape.index(max(values.shape))
    beside = index_at[:widest] + [(index_at[widest] + 1) % values.shape[widest]] + index_at[widest + 1:]
    return values.at[tuple(index_at)].set(least).at[tuple(beside)].set(top_value)


def setup_inputs(seed: int = 0) -> dict:
    arg_keys = jax.random.split(jax.random.key(seed), 4)
    queries = draw_queries(jax.random.fold_in(arg_keys[3], 71), 0)
    candidates = draw_candidates(jax.random.fold_in(arg_keys[3], 71), 0)
    targets = plant(jax.random.randint(arg_keys[2], (QUERIES,), 0, CANDS), jax.random.fold_in(arg_keys[2], 1), 0, CANDS - 1).astype(jnp.int32)
    return dict(queries=queries, candidates=candidates, targets=targets)


def reference(queries, candidates, targets):
    blocks = candidates.reshape(N_GROUP * N_SHARD, CAND_DEV, D)

    def step(carry, block):
        top, total = carry
        scores = jnp.dot(queries, block.T, preferred_element_type=jnp.float32)
        block_top = jnp.max(scores, axis=1)
        new_top = jnp.maximum(top, block_top)
        total = total * jnp.exp(top - new_top) + jnp.sum(jnp.exp(scores - new_top[:, None]), axis=1)
        return (new_top, total), None

    start = (jnp.full((QUERIES,), -jnp.inf, jnp.float32), jnp.zeros((QUERIES,), jnp.float32))
    (top, total), unused = lax.scan(step, start, blocks)
    chosen = jnp.take(candidates, targets.astype(jnp.int32), axis=0)
    picked = jnp.sum(queries.astype(jnp.float32) * chosen.astype(jnp.float32), axis=1)
    losses = top + jnp.log(total) - picked
    return losses, jnp.mean(losses)
```

```python
import functools

import jax
import jax.numpy as jnp
from jax import lax
from jax.experimental import pallas as pl
from jax.experimental.pallas import tpu as pltpu
from jax.sharding import Mesh
from jax.sharding import PartitionSpec as P

SHARD = ("x", "y", "core")
EVERY = ("group",) + SHARD
MESH = pl.DeviceIdType.MESH
NZ, NX, NY = 8, 4, 4
PLANE = NX * NY * 2
LANES = 128
CHUNK = 256
ROWS = 1024
LOWEST = -3.0e38

SLOTS = (
    ("o", 0, 0), ("o", 1, 0), ("o", 3, 0), ("o", 0, 1), ("o", 0, 3), ("m", 0, 0),
    ("o", 2, 0), ("m", 1, 0), ("m", 3, 0), ("m", 0, 1), ("m", 0, 3),
    ("m", 2, 0), ("o", 1, 1), ("o", 3, 1), ("o", 1, 3), ("o", 3, 3),
    ("o", 2, 1), ("o", 2, 3), ("m", 1, 1), ("m", 3, 1), ("m", 1, 3), ("m", 3, 3),
    ("m", 2, 1), ("m", 2, 3), ("o", 0, 2), ("o", 1, 2), ("o", 2, 2),
    ("o", 3, 2), ("m", 0, 2), ("m", 1, 2), ("m", 2, 2), ("m", 3, 2),
)
PLACE = {slot: k for k, slot in enumerate(SLOTS)}
ARRIVALS = {
    (0, 0): (("o", 1, 0), ("o", 3, 0), ("o", 0, 1), ("o", 0, 3), ("m", 0, 0)),
    (0, 2): (("o", 2, 0),),
    (1, 0): (("m", 1, 0), ("m", 3, 0), ("m", 0, 1), ("m", 0, 3)),
    (1, 2): (("o", 1, 1), ("o", 3, 1), ("o", 1, 3), ("o", 3, 3)),
    (2, 0): (("m", 2, 0),),
    (2, 2): (("o", 2, 1), ("o", 2, 3)),
    (3, 0): (("m", 1, 1), ("m", 3, 1), ("m", 1, 3), ("m", 3, 3)),
    (3, 2): (("o", 0, 2), ("o", 1, 2)),
    (4, 0): (("m", 2, 1), ("m", 2, 3), ("o", 2, 2)),
    (4, 2): (("o", 3, 2),),
    (5, 0): (("m", 0, 2), ("m", 1, 2), ("m", 2, 2), ("m", 3, 2)),
}


def folded(block, count, top, total, picked, wanted, first):
    tops = [top, None, None, None]
    for r in range(count):
        v = block[8 * r : 8 * r + 8, :]
        tops[r % 4] = v if tops[r % 4] is None else jnp.maximum(tops[r % 4], v)
    new = jnp.maximum(jnp.maximum(tops[0], tops[1]), jnp.maximum(tops[2], tops[3]))
    sums = [total * jnp.exp(top - new), None, None, None]
    for r in range(count):
        v = block[8 * r : 8 * r + 8, :]
        e = jnp.exp(v - new)
        sums[r % 4] = e if sums[r % 4] is None else sums[r % 4] + e
        picked = jnp.where(wanted == first + r, v, picked)
    return new, (sums[0] + sums[1]) + (sums[2] + sums[3]), picked


def merged(pieces):
    top = jnp.max(pieces[:, 0:1, :], axis=0)
    total = jnp.sum(jnp.exp(pieces[:, 0:1, :] - top[None]), axis=0)
    return top + jnp.log(total), jnp.sum(pieces[:, 1:2, :], axis=0)


def kernel(
    q_ref, t_ref, c_hbm, out_ref,
    zbuf, qall, cbuf, sbuf, trel, res, part, inbox, zin, outall,
    c_sem, zs_sem, zr_sem, send_sem, own_sem, mate_sem,
    rs_sem, rr_sem, gs_sem, gr_sem, as_sem, ar_sem,
):
    z, x, y, c = (lax.axis_index(a) for a in EVERY)
    per = q_ref.shape[0]
    block = NZ * per
    n_cand = cbuf.shape[0]
    steps = n_cand // ROWS
    me = (x * NY + y) * 2 + c
    base = (z * PLANE + me) * n_cand

    loads = [
        pltpu.make_async_copy(
            c_hbm.at[pl.ds(b * ROWS, ROWS)], cbuf.at[pl.ds(b * ROWS, ROWS)], c_sem.at[b]
        )
        for b in range(steps)
    ]
    for load in loads:
        load.start()

    def plane_id(r):
        return {"x": r // (NY * 2), "y": (r // 2) % NY, "core": r % 2}

    barrier = pltpu.get_barrier_semaphore()

    @pl.loop(1, NZ)
    def _(o):
        pl.semaphore_signal(barrier, inc=1, device_id={"group": (z + o) % NZ}, device_id_type=MESH)

    @pl.loop(1, PLANE)
    def _(o):
        pl.semaphore_signal(barrier, inc=1, device_id=plane_id((me + o) % PLANE), device_id_type=MESH)

    pl.semaphore_wait(barrier, NZ - 1 + PLANE - 1)

    def along(o):
        return pltpu.make_async_remote_copy(
            src_ref=q_ref, dst_ref=zbuf.at[z], send_sem=zs_sem.at[o], recv_sem=zr_sem.at[z],
            device_id={"group": (z + o) % NZ}, device_id_type=MESH,
        )

    def along_in(o):
        other = (z + o) % NZ
        return pltpu.make_async_remote_copy(
            src_ref=q_ref, dst_ref=zbuf.at[other], send_sem=zs_sem.at[o], recv_sem=zr_sem.at[other],
            device_id={"group": other}, device_id_type=MESH,
        )

    for o in range(1, NZ):
        along(o).start()
    zbuf[pl.ds(z, 1)] = q_ref[...][None]

    def source_row(slot):
        kind, da, db = slot
        cs = c if kind == "o" else 1 - c
        xs = (x + da * (1 - cs) + db * cs) % NX
        ys = (y + da * cs + db * (1 - cs)) % NY
        return (xs * NY + ys) * 2 + cs

    rows = [source_row(slot) for slot in SLOTS]
    for k in range(PLANE):
        trel[:, k * block : (k + 1) * block] = t_ref[rows[k]][:, :block]

    for o in range(1, NZ):
        along_in(o).wait_recv()
    qall[0:block, :] = jnp.concatenate(
        [zbuf[k].astype(jnp.float32) for k in range(NZ)], axis=0
    ).astype(qall.dtype)

    sent = []

    def at(slot):
        return qall.at[pl.ds(PLACE[slot] * block, block)]

    def copy(src, dst, device, sem):
        op = pltpu.make_async_remote_copy(
            src_ref=at(src), dst_ref=at(dst), send_sem=send_sem.at[len(sent)], recv_sem=sem,
            device_id=device, device_id_type=MESH,
        )
        op.start()
        sent.append(op)

    def over(src, ea, eb):
        _, da, db = src
        to = ("o", (da - ea) % 4, (db - eb) % 4)
        device = {
            "x": (x + ea * (1 - c) + eb * c) % NX,
            "y": (y + ea * c + eb * (1 - c)) % NY,
        }
        copy(src, to, device, own_sem.at[to[1] * 4 + to[2]])

    def across(src):
        _, da, db = src
        copy(src, ("m", da, db), {"core": 1 - c}, mate_sem.at[da * 4 + db])

    def arrived(slot):
        kind, da, db = slot
        sem = own_sem if kind == "o" else mate_sem
        pltpu.make_async_remote_copy(
            src_ref=at(slot), dst_ref=at(slot), send_sem=send_sem.at[0], recv_sem=sem.at[da * 4 + db],
            device_id={"core": 1 - c}, device_id_type=MESH,
        ).wait_recv()

    def passed_on(slot):
        kind, da, db = slot
        if kind == "m":
            return
        if db == 0:
            over(slot, 0, 1)
            over(slot, 0, -1)
        if db == 1 and da in (2, 3):
            over(slot, 0, -1)
        if db == 3 and da in (0, 1):
            over(slot, 0, 1)
        across(slot)

    mine = ("o", 0, 0)
    over(mine, 1, 0)
    over(mine, -1, 0)
    passed_on(mine)
    over(mine, 2, 0)

    def fresh():
        return (
            jnp.full((8, CHUNK), LOWEST, jnp.float32),
            jnp.zeros((8, CHUNK), jnp.float32),
            jnp.zeros((8, CHUNK), jnp.float32),
        )

    state = fresh()
    pending = None
    chunks = qall.shape[0] // CHUNK

    def drained(pending, state):
        k, b, side = pending
        mark = trel[:, k * CHUNK : (k + 1) * CHUNK] - base
        wanted = jnp.broadcast_to(mark >> 3, (8, CHUNK))
        state = folded(sbuf.at[side], ROWS // 8, *state, wanted, b * (ROWS // 8))
        if b < steps - 1:
            return state
        top, total, picked = state
        best = jnp.max(top, axis=0, keepdims=True)
        whole = jnp.sum(total * jnp.exp(top - best), axis=0, keepdims=True)
        line = lax.broadcasted_iota(jnp.int32, (8, CHUNK), 0)
        hit = jnp.where(line == (mark & 7), picked, 0.0)
        res[0:1, k * CHUNK : (k + 1) * CHUNK] = best + jnp.log(whole)
        res[1:2, k * CHUNK : (k + 1) * CHUNK] = jnp.sum(hit, axis=0, keepdims=True)
        return fresh()

    for k in range(chunks):
        for b in range(steps):
            if k == 0:
                loads[b].wait()
            for slot in ARRIVALS.get((k, b), ()):
                arrived(slot)
                passed_on(slot)
            side = (k * steps + b) % 2
            sbuf[side] = lax.dot_general(
                cbuf[b * ROWS : (b + 1) * ROWS, :], qall[k * CHUNK : (k + 1) * CHUNK, :],
                (((1,), (1,)), ((), ())), preferred_element_type=jnp.float32,
            )
            if pending is not None:
                state = drained(pending, state)
            pending = (k, b, side)
    drained(pending, state)

    for k in range(PLANE):
        part[rows[k], :, 0:block] = res[:, k * block : (k + 1) * block]

    def gathered(src, dst, s_sem, r_sem):
        def op(o, at_me):
            other = (me + o) % PLANE
            slot = me if at_me else other
            return pltpu.make_async_remote_copy(
                src_ref=src(other), dst_ref=dst.at[slot], send_sem=s_sem.at[o], recv_sem=r_sem.at[slot],
                device_id=plane_id(other), device_id_type=MESH,
            )

        @pl.loop(1, PLANE)
        def _(o):
            op(o, True).start()

        @pl.loop(1, PLANE)
        def _(o):
            op(o, False).wait_recv()

        return op

    inbox[pl.ds(me, 1)] = part[pl.ds(me, 1)]
    scattered = gathered(lambda other: part.at[other], inbox, rs_sem, rr_sem)
    lse, picked = merged(inbox[...])

    zin[pl.ds(z, 1), 0:1, :] = lse[None]
    zin[pl.ds(z, 1), 1:2, :] = picked[None]

    def reduce_to(o, at_me):
        other = (z + o) % NZ
        slot = z if at_me else other
        return pltpu.make_async_remote_copy(
            src_ref=zin.at[z], dst_ref=zin.at[slot], send_sem=gs_sem.at[o], recv_sem=gr_sem.at[slot],
            device_id={"group": other}, device_id_type=MESH,
        )

    for o in range(1, NZ):
        reduce_to(o, True).start()
    for o in range(1, NZ):
        reduce_to(o, False).wait_recv()
    lse, picked = merged(zin[...])

    outall[pl.ds(me, 1)] = (lse - picked)[None]
    spread = gathered(lambda other: outall.at[me], outall, as_sem, ar_sem)
    out_ref[...] = outall[...]

    for o in range(1, NZ):
        along(o).wait_send()
        reduce_to(o, True).wait_send()
    for op in sent:
        op.wait_send()

    @pl.loop(1, PLANE)
    def _(o):
        scattered(o, True).wait_send()
        spread(o, True).wait_send()


def on_device(queries, candidates, targets):
    per, width = queries.shape
    block = NZ * per
    total = block * PLANE
    marks = targets.reshape(NZ, PLANE, per).transpose(1, 0, 2).reshape(PLANE, 1, block)
    marks = jnp.pad(marks, ((0, 0), (0, 0), (0, LANES - block)))
    DMA = pltpu.SemaphoreType.DMA
    out = pl.pallas_call(
        kernel,
        out_shape=jax.ShapeDtypeStruct((PLANE, 1, LANES), jnp.float32),
        in_specs=[
            pl.BlockSpec(memory_space=pltpu.VMEM),
            pl.BlockSpec(memory_space=pltpu.VMEM),
            pl.BlockSpec(memory_space=pl.ANY),
        ],
        out_specs=pl.BlockSpec(memory_space=pltpu.VMEM),
        scratch_shapes=[
            pltpu.VMEM((NZ, per, width), jnp.bfloat16),
            pltpu.VMEM((total, width), jnp.bfloat16),
            pltpu.VMEM(candidates.shape, jnp.bfloat16),
            pltpu.VMEM((2, ROWS, CHUNK), jnp.float32),
            pltpu.VMEM((1, total), jnp.int32),
            pltpu.VMEM((2, total), jnp.float32),
            pltpu.VMEM((PLANE, 2, LANES), jnp.float32),
            pltpu.VMEM((PLANE, 2, LANES), jnp.float32),
            pltpu.VMEM((NZ, 2, LANES), jnp.float32),
            pltpu.VMEM((PLANE, 1, LANES), jnp.float32),
            DMA((candidates.shape[0] // ROWS,)),
            DMA((NZ,)),
            DMA((NZ,)),
            DMA((31,)),
            DMA((16,)),
            DMA((16,)),
            DMA((PLANE,)),
            DMA((PLANE,)),
            DMA((NZ,)),
            DMA((NZ,)),
            DMA((PLANE,)),
            DMA((PLANE,)),
        ],
        compiler_params=pltpu.CompilerParams(
            collective_id=0, has_side_effects=True, vmem_limit_bytes=56 * 2**20
        ),
    )(queries, marks, candidates)
    losses = out[:, 0, :block].reshape(PLANE, NZ, per).transpose(1, 0, 2).reshape(total)
    return losses, jnp.mean(losses)


def solution(mesh):
    finer = Mesh(mesh.devices.reshape(mesh.shape["group"], NX, NY, 2), EVERY)
    return jax.shard_map(
        on_device,
        mesh=finer,
        in_specs=(P(EVERY, None), P(EVERY, None), P()),
        out_specs=(P(), P()),
        check_vma=False,
    )
```

```python
import functools

import jax
import jax.numpy as jnp
from jax import lax
from jax.experimental import pallas as pl
from jax.experimental.pallas import tpu as pltpu
from jax.sharding import Mesh
from jax.sharding import PartitionSpec as P

SHARD = ("x", "y", "core")
EVERY = ("group",) + SHARD
MESH = pl.DeviceIdType.MESH
NZ, NX, NY = 8, 4, 4
PLANE = NX * NY * 2
LANES = 128
CHUNK = 256
ROWS = 1024
LOWEST = -3.0e38
AROUND = sorted(
    ((dx, dy, dc) for dx in range(NX) for dy in range(NY) for dc in range(2) if dx or dy or dc),
    key=lambda d: -(min(d[0], NX - d[0]) + min(d[1], NY - d[1])),
)
ALONG = sorted(range(1, NZ), key=lambda o: -min(o, NZ - o))

SLOTS = (
    ("o", 0, 0), ("o", 1, 0), ("o", 3, 0), ("o", 0, 1), ("o", 0, 3), ("m", 0, 0),
    ("o", 2, 0), ("m", 1, 0), ("m", 3, 0), ("m", 0, 1), ("m", 0, 3),
    ("m", 2, 0), ("o", 1, 1), ("o", 3, 1), ("o", 1, 3), ("o", 3, 3),
    ("o", 2, 1), ("o", 2, 3), ("m", 1, 1), ("m", 3, 1), ("m", 1, 3), ("m", 3, 3),
    ("m", 2, 1), ("m", 2, 3), ("o", 0, 2), ("o", 1, 2), ("o", 2, 2),
    ("o", 3, 2), ("m", 0, 2), ("m", 1, 2), ("m", 2, 2), ("m", 3, 2),
)
PLACE = {slot: k for k, slot in enumerate(SLOTS)}
ARRIVALS = {
    (0, 0): (("o", 1, 0), ("o", 3, 0), ("o", 0, 1), ("o", 0, 3), ("m", 0, 0)),
    (0, 2): (("o", 2, 0),),
    (1, 0): (("m", 1, 0), ("m", 3, 0), ("m", 0, 1), ("m", 0, 3)),
    (1, 2): (("o", 1, 1), ("o", 3, 1), ("o", 1, 3), ("o", 3, 3)),
    (2, 0): (("m", 2, 0),),
    (2, 2): (("o", 2, 1), ("o", 2, 3)),
    (3, 0): (("m", 1, 1), ("m", 3, 1), ("m", 1, 3), ("m", 3, 3)),
    (3, 2): (("o", 0, 2), ("o", 1, 2)),
    (4, 0): (("m", 2, 1), ("m", 2, 3), ("o", 2, 2)),
    (4, 2): (("o", 3, 2),),
    (5, 0): (("m", 0, 2), ("m", 1, 2), ("m", 2, 2), ("m", 3, 2)),
}


def folded(block, count, top, total, picked, wanted, first):
    tops = [top, None, None, None]
    for r in range(count):
        v = block[8 * r : 8 * r + 8, :]
        tops[r % 4] = v if tops[r % 4] is None else jnp.maximum(tops[r % 4], v)
    new = jnp.maximum(jnp.maximum(tops[0], tops[1]), jnp.maximum(tops[2], tops[3]))
    sums = [total * jnp.exp(top - new), None, None, None]
    for r in range(count):
        v = block[8 * r : 8 * r + 8, :]
        e = jnp.exp(v - new)
        sums[r % 4] = e if sums[r % 4] is None else sums[r % 4] + e
        picked = jnp.where(wanted == first + r, v, picked)
    return new, (sums[0] + sums[1]) + (sums[2] + sums[3]), picked


def merged(pieces):
    top = jnp.max(pieces[:, 0:1, :], axis=0)
    total = jnp.sum(jnp.exp(pieces[:, 0:1, :] - top[None]), axis=0)
    return top + jnp.log(total), jnp.sum(pieces[:, 1:2, :], axis=0)


def kernel(
    q_ref, t_ref, c_hbm, out_ref, mean_ref,
    zbuf, qall, cbuf, sbuf, pmat, own, tbuf, trel, res, part, inbox, zin, outall,
    c_sem, zs_sem, zr_sem, send_sem, own_sem, mate_sem,
    rs_sem, rr_sem, gs_sem, gr_sem, as_sem, ar_sem,
):
    z, x, y, c = (lax.axis_index(a) for a in EVERY)
    per = q_ref.shape[0]
    block = NZ * per
    n_cand = cbuf.shape[1]
    tiles = cbuf.shape[0]
    steps = n_cand // ROWS
    me = (x * NY + y) * 2 + c
    base = (z * PLANE + me) * n_cand

    loads = [
        pltpu.make_async_copy(
            c_hbm.at[:, pl.ds(j * LANES, LANES)], cbuf.at[j], c_sem.at[j]
        )
        for j in range(tiles)
    ]
    for load in loads:
        load.start()

    def plane_id(r):
        return {"x": r // (NY * 2), "y": (r // 2) % NY, "core": r % 2}

    barrier = pltpu.get_barrier_semaphore()

    @pl.loop(1, NZ)
    def _(o):
        pl.semaphore_signal(barrier, inc=1, device_id={"group": (z + o) % NZ}, device_id_type=MESH)

    @pl.loop(1, PLANE)
    def _(o):
        pl.semaphore_signal(barrier, inc=1, device_id=plane_id((me + o) % PLANE), device_id_type=MESH)

    count = t_ref.shape[1]
    g = lax.broadcasted_iota(jnp.int32, (1, count), 1).astype(jnp.float32)
    gz = jnp.floor((2.0 * g + 1.0) * (0.5 / (PLANE * per)))
    within = g - gz * (PLANE * per)
    row = jnp.floor((2.0 * within + 1.0) * (0.5 / per))
    lane = (gz * per + within - row * per).astype(jnp.int32)
    row = row.astype(jnp.int32)
    at_lane = lax.broadcasted_iota(jnp.int32, (LANES, count), 0) == lane
    pmat[...] = jnp.where(at_lane, 1.0, 0.0).astype(pmat.dtype)
    at_row = lax.broadcasted_iota(jnp.int32, (PLANE, count), 0) == row
    own[...] = jnp.where(at_row, 1.0, 0.0)

    t = t_ref[...]
    pieces = jnp.concatenate(
        [own[...] * p.astype(jnp.float32) for p in (t & 255, (t >> 8) & 255, t >> 16)], axis=0
    ).astype(pmat.dtype)
    table = lax.dot_general(
        pieces, pmat[...], (((1,), (1,)), ((), ())), preferred_element_type=jnp.float32
    )
    tbuf[...] = (
        table[0:PLANE] + 256.0 * table[PLANE : 2 * PLANE] + 65536.0 * table[2 * PLANE :]
    ).astype(jnp.int32)

    def source_row(slot):
        kind, da, db = slot
        cs = c if kind == "o" else 1 - c
        xs = (x + da * (1 - cs) + db * cs) % NX
        ys = (y + da * cs + db * (1 - cs)) % NY
        return (xs * NY + ys) * 2 + cs

    rows = [source_row(slot) for slot in SLOTS]
    for k in range(PLANE):
        trel[:, k * block : (k + 1) * block] = tbuf[pl.ds(rows[k], 1), :][:, :block]

    pl.semaphore_wait(barrier, NZ - 1 + PLANE - 1)

    def along(o):
        return pltpu.make_async_remote_copy(
            src_ref=q_ref, dst_ref=zbuf.at[z], send_sem=zs_sem.at[o], recv_sem=zr_sem.at[z],
            device_id={"group": (z + o) % NZ}, device_id_type=MESH,
        )

    def along_in(o):
        other = (z + o) % NZ
        return pltpu.make_async_remote_copy(
            src_ref=q_ref, dst_ref=zbuf.at[other], send_sem=zs_sem.at[o], recv_sem=zr_sem.at[other],
            device_id={"group": other}, device_id_type=MESH,
        )

    for o in ALONG:
        along(o).start()
    zbuf[pl.ds(z, 1)] = q_ref[...][None]

    for o in ALONG:
        along_in(o).wait_recv()
    column = jnp.concatenate(
        [zbuf[k].astype(jnp.float32) for k in range(NZ)], axis=0
    ).astype(qall.dtype)
    for j in range(tiles):
        qall[0, j] = column[:, j * LANES : (j + 1) * LANES]

    sent = []

    def at(slot):
        return qall.at[PLACE[slot]]

    def copy(src, dst, device, sem):
        op = pltpu.make_async_remote_copy(
            src_ref=at(src), dst_ref=at(dst), send_sem=send_sem.at[len(sent)], recv_sem=sem,
            device_id=device, device_id_type=MESH,
        )
        op.start()
        sent.append(op)

    def over(src, ea, eb):
        _, da, db = src
        to = ("o", (da - ea) % 4, (db - eb) % 4)
        device = {
            "x": (x + ea * (1 - c) + eb * c) % NX,
            "y": (y + ea * c + eb * (1 - c)) % NY,
        }
        copy(src, to, device, own_sem.at[to[1] * 4 + to[2]])

    def across(src):
        _, da, db = src
        copy(src, ("m", da, db), {"core": 1 - c}, mate_sem.at[da * 4 + db])

    def arrived(slot):
        kind, da, db = slot
        sem = own_sem if kind == "o" else mate_sem
        pltpu.make_async_remote_copy(
            src_ref=at(slot), dst_ref=at(slot), send_sem=send_sem.at[0], recv_sem=sem.at[da * 4 + db],
            device_id={"core": 1 - c}, device_id_type=MESH,
        ).wait_recv()

    def passed_on(slot):
        kind, da, db = slot
        if kind == "m":
            return
        if db == 0:
            over(slot, 0, 1)
            over(slot, 0, -1)
        if db == 1 and da in (2, 3):
            over(slot, 0, -1)
        if db == 3 and da in (0, 1):
            over(slot, 0, 1)
        across(slot)

    mine = ("o", 0, 0)
    over(mine, 2, 0)
    over(mine, 1, 0)
    over(mine, -1, 0)
    passed_on(mine)

    def fresh():
        return (
            jnp.full((8, CHUNK), LOWEST, jnp.float32),
            jnp.zeros((8, CHUNK), jnp.float32),
            jnp.zeros((8, CHUNK), jnp.float32),
        )

    state = fresh()
    pending = None
    chunks = PLANE * block // CHUNK
    groups = block // 16

    def candidates_of(b):
        return jnp.concatenate(
            [cbuf[j, b * ROWS : (b + 1) * ROWS, :] for j in range(tiles)], axis=1
        )

    def queries_of(k):
        places = [divmod(k * CHUNK // 16 + i, groups) for i in range(CHUNK // 16)]
        return jnp.concatenate(
            [
                jnp.concatenate([qall[p, j, 16 * i : 16 * i + 16, :] for p, i in places], axis=0)
                for j in range(tiles)
            ],
            axis=1,
        )

    def drained(pending, state):
        k, b, side = pending
        mark = trel[:, k * CHUNK : (k + 1) * CHUNK] - base
        wanted = jnp.broadcast_to(mark >> 3, (8, CHUNK))
        state = folded(sbuf.at[side], ROWS // 8, *state, wanted, b * (ROWS // 8))
        if b < steps - 1:
            return state
        top, total, picked = state
        best = jnp.max(top, axis=0, keepdims=True)
        whole = jnp.sum(total * jnp.exp(top - best), axis=0, keepdims=True)
        line = lax.broadcasted_iota(jnp.int32, (8, CHUNK), 0)
        hit = jnp.where(line == (mark & 7), picked, 0.0)
        res[0:1, k * CHUNK : (k + 1) * CHUNK] = best + jnp.log(whole)
        res[1:2, k * CHUNK : (k + 1) * CHUNK] = jnp.sum(hit, axis=0, keepdims=True)
        return fresh()

    for load in loads:
        load.wait()
    for k in range(chunks):
        for b in range(steps):
            for slot in ARRIVALS.get((k, b), ()):
                arrived(slot)
                passed_on(slot)
            side = (k * steps + b) % 2
            sbuf[side] = lax.dot_general(
                candidates_of(b), queries_of(k),
                (((1,), (1,)), ((), ())), preferred_element_type=jnp.float32,
            )
            if pending is not None:
                state = drained(pending, state)
            pending = (k, b, side)
    drained(pending, state)

    for k in range(PLANE):
        part[rows[k], :, 0:block] = res[:, k * block : (k + 1) * block]

    def gathered(src, dst, s_sem, r_sem):
        ops = []
        for k, (dx, dy, dc) in enumerate(AROUND):
            device = {"x": (x + dx) % NX, "y": (y + dy) % NY, "core": (c + dc) % 2}
            other = (device["x"] * NY + device["y"]) * 2 + device["core"]
            op, back = (
                pltpu.make_async_remote_copy(
                    src_ref=src(other), dst_ref=dst.at[slot], send_sem=s_sem.at[k],
                    recv_sem=r_sem.at[slot], device_id=device, device_id_type=MESH,
                )
                for slot in (me, other)
            )
            op.start()
            ops.append((op, back))
        for _, back in ops:
            back.wait_recv()
        return ops

    inbox[pl.ds(me, 1)] = part[pl.ds(me, 1)]
    scattered = gathered(lambda other: part.at[other], inbox, rs_sem, rr_sem)
    lse, picked = merged(inbox[...])

    zin[pl.ds(z, 1), 0:1, :] = lse[None]
    zin[pl.ds(z, 1), 1:2, :] = picked[None]

    def reduce_to(o, at_me):
        other = (z + o) % NZ
        slot = z if at_me else other
        return pltpu.make_async_remote_copy(
            src_ref=zin.at[z], dst_ref=zin.at[slot], send_sem=gs_sem.at[o], recv_sem=gr_sem.at[slot],
            device_id={"group": other}, device_id_type=MESH,
        )

    for o in ALONG:
        reduce_to(o, True).start()
    for o in ALONG:
        reduce_to(o, False).wait_recv()
    lse, picked = merged(zin[...])

    outall[pl.ds(me, 1)] = (lse - picked)[None]
    spread = gathered(lambda other: outall.at[me], outall, as_sem, ar_sem)
    lanes = lax.broadcasted_iota(jnp.int32, (PLANE, LANES), 1)
    value = jnp.concatenate([outall[k] for k in range(PLANE)], axis=0)
    value = jnp.where(lanes < block, value, 0.0)
    high = value.astype(pmat.dtype)
    rest = value - high.astype(jnp.float32)
    middle = rest.astype(pmat.dtype)
    low = (rest - middle.astype(jnp.float32)).astype(pmat.dtype)
    spreads = jnp.dot(
        jnp.concatenate([high, middle, low], axis=0), pmat[...], preferred_element_type=jnp.float32
    )
    value = spreads[0:PLANE] + spreads[PLANE : 2 * PLANE] + spreads[2 * PLANE :]
    losses = jnp.sum(own[...] * value, axis=0, keepdims=True)
    out_ref[...] = losses
    mean_ref[0, 0] = jnp.sum(losses) / count

    for o in ALONG:
        along(o).wait_send()
        reduce_to(o, True).wait_send()
    for op in sent:
        op.wait_send()

    for op, _ in scattered + spread:
        op.wait_send()


def on_device(queries, candidates, targets):
    per, width = queries.shape
    block = NZ * per
    total = block * PLANE
    DMA = pltpu.SemaphoreType.DMA
    losses, mean = pl.pallas_call(
        kernel,
        out_shape=(
            jax.ShapeDtypeStruct((1, total), jnp.float32),
            jax.ShapeDtypeStruct((1, 1), jnp.float32),
        ),
        in_specs=[
            pl.BlockSpec(memory_space=pltpu.VMEM),
            pl.BlockSpec(memory_space=pltpu.VMEM),
            pl.BlockSpec(memory_space=pl.ANY),
        ],
        out_specs=(
            pl.BlockSpec(memory_space=pltpu.VMEM),
            pl.BlockSpec(memory_space=pltpu.SMEM),
        ),
        scratch_shapes=[
            pltpu.VMEM((NZ, per, width), jnp.bfloat16),
            pltpu.VMEM((PLANE, width // LANES, block, LANES), jnp.bfloat16),
            pltpu.VMEM((width // LANES, candidates.shape[0], LANES), jnp.bfloat16),
            pltpu.VMEM((2, ROWS, CHUNK), jnp.float32),
            pltpu.VMEM((LANES, total), jnp.bfloat16),
            pltpu.VMEM((PLANE, total), jnp.float32),
            pltpu.VMEM((PLANE, LANES), jnp.int32),
            pltpu.VMEM((1, total), jnp.int32),
            pltpu.VMEM((2, total), jnp.float32),
            pltpu.VMEM((PLANE, 2, LANES), jnp.float32),
            pltpu.VMEM((PLANE, 2, LANES), jnp.float32),
            pltpu.VMEM((NZ, 2, LANES), jnp.float32),
            pltpu.VMEM((PLANE, 1, LANES), jnp.float32),
            DMA((width // LANES,)),
            DMA((NZ,)),
            DMA((NZ,)),
            DMA((31,)),
            DMA((16,)),
            DMA((16,)),
            DMA((PLANE,)),
            DMA((PLANE,)),
            DMA((NZ,)),
            DMA((NZ,)),
            DMA((PLANE,)),
            DMA((PLANE,)),
        ],
        compiler_params=pltpu.CompilerParams(
            collective_id=0, has_side_effects=True, vmem_limit_bytes=56 * 2**20
        ),
    )(queries, targets.reshape(1, total), candidates)
    return losses.reshape(total), mean.reshape(())


def solution(mesh):
    finer = Mesh(mesh.devices.reshape(mesh.shape["group"], NX, NY, 2), EVERY)
    return jax.shard_map(
        on_device,
        mesh=finer,
        in_specs=(P(EVERY, None), P(EVERY, None), P()),
        out_specs=(P(), P()),
        check_vma=False,
    )
```

```python
import functools

import jax
import jax.numpy as jnp
from jax import lax
from jax.experimental import pallas as pl
from jax.experimental.pallas import tpu as pltpu
from jax.sharding import Mesh
from jax.sharding import PartitionSpec as P

SHARD = ("x", "y", "core")
EVERY = ("group",) + SHARD
MESH = pl.DeviceIdType.MESH
NZ, NX, NY = 8, 4, 4
PLANE = NX * NY * 2
LANES = 128
CHUNK = 256
ROWS = 1024
LOWEST = -3.0e38
AROUND = sorted(
    ((dx, dy, dc) for dx in range(NX) for dy in range(NY) for dc in range(2) if dx or dy or dc),
    key=lambda d: -(min(d[0], NX - d[0]) + min(d[1], NY - d[1])),
)
ALONG = sorted(range(1, NZ), key=lambda o: -min(o, NZ - o))

SLOTS = (
    ("o", 0, 0), ("m", 0, 0), ("o", 1, 0), ("o", 3, 0), ("m", 1, 0), ("m", 3, 0),
    ("o", 0, 1), ("o", 0, 3), ("m", 0, 1), ("m", 0, 3), ("o", 2, 0),
    ("m", 2, 0), ("o", 1, 1), ("o", 3, 1), ("o", 1, 3), ("o", 3, 3),
    ("o", 2, 1), ("o", 2, 3), ("m", 1, 1), ("m", 3, 1), ("m", 1, 3), ("m", 3, 3),
    ("m", 2, 1), ("m", 2, 3), ("o", 0, 2), ("o", 1, 2), ("m", 0, 2),
    ("o", 3, 2), ("m", 1, 2), ("o", 2, 2), ("m", 3, 2), ("m", 2, 2),
)
PLACE = {slot: k for k, slot in enumerate(SLOTS)}
ARRIVALS = {
    (0, 0): (("o", 1, 0), ("o", 3, 0), ("m", 1, 0), ("m", 3, 0)),
    (0, 2): (("o", 0, 1), ("o", 0, 3)),
    (1, 0): (("m", 0, 1), ("m", 0, 3), ("o", 2, 0)),
    (1, 2): (("o", 1, 1), ("o", 3, 1), ("o", 1, 3), ("o", 3, 3)),
    (2, 0): (("m", 2, 0),),
    (2, 2): (("o", 0, 2), ("o", 2, 1), ("o", 2, 3)),
    (3, 0): (("m", 1, 1), ("m", 3, 1), ("m", 1, 3), ("m", 3, 3)),
    (3, 2): (("o", 1, 2), ("o", 3, 2)),
    (4, 0): (("m", 2, 1), ("m", 2, 3), ("m", 0, 2)),
    (4, 2): (("o", 2, 2),),
    (5, 0): (("m", 1, 2), ("m", 3, 2), ("m", 2, 2)),
}


def folded(block, count, top, total, picked, wanted, first):
    tops = [top, None, None, None]
    for r in range(count):
        v = block[8 * r : 8 * r + 8, :]
        tops[r % 4] = v if tops[r % 4] is None else jnp.maximum(tops[r % 4], v)
    new = jnp.maximum(jnp.maximum(tops[0], tops[1]), jnp.maximum(tops[2], tops[3]))
    sums = [total * jnp.exp(top - new), None, None, None]
    for r in range(count):
        v = block[8 * r : 8 * r + 8, :]
        e = jnp.exp(v - new)
        sums[r % 4] = e if sums[r % 4] is None else sums[r % 4] + e
        picked = jnp.where(wanted == first + r, v, picked)
    return new, (sums[0] + sums[1]) + (sums[2] + sums[3]), picked


def merged(pieces):
    top = jnp.max(pieces[:, 0:1, :], axis=0)
    total = jnp.sum(jnp.exp(pieces[:, 0:1, :] - top[None]), axis=0)
    return top + jnp.log(total), jnp.sum(pieces[:, 1:2, :], axis=0)


def kernel(
    q_ref, t_ref, c_hbm, out_ref, mean_ref,
    zbuf, qall, cbuf, sbuf, pmat, own, tbuf, trel, res, part, inbox, zin, outall,
    c_sem, zs_sem, zr_sem, send_sem, own_sem, mate_sem,
    rs_sem, rr_sem, gs_sem, gr_sem, as_sem, ar_sem,
):
    z, x, y, c = (lax.axis_index(a) for a in EVERY)
    per = q_ref.shape[0]
    block = NZ * per
    n_cand = cbuf.shape[1]
    tiles = cbuf.shape[0]
    steps = n_cand // ROWS
    me = (x * NY + y) * 2 + c
    base = (z * PLANE + me) * n_cand

    loads = [
        pltpu.make_async_copy(
            c_hbm.at[:, pl.ds(j * LANES, LANES)], cbuf.at[j], c_sem.at[j]
        )
        for j in range(tiles)
    ]
    for load in loads:
        load.start()

    def plane_id(r):
        return {"x": r // (NY * 2), "y": (r // 2) % NY, "core": r % 2}

    barrier = pltpu.get_barrier_semaphore()

    @pl.loop(1, NZ)
    def _(o):
        pl.semaphore_signal(barrier, inc=1, device_id={"group": (z + o) % NZ}, device_id_type=MESH)

    @pl.loop(1, PLANE)
    def _(o):
        pl.semaphore_signal(barrier, inc=1, device_id=plane_id((me + o) % PLANE), device_id_type=MESH)

    count = t_ref.shape[1]
    g = lax.broadcasted_iota(jnp.int32, (1, count), 1).astype(jnp.float32)
    gz = jnp.floor((2.0 * g + 1.0) * (0.5 / (PLANE * per)))
    within = g - gz * (PLANE * per)
    row = jnp.floor((2.0 * within + 1.0) * (0.5 / per))
    lane = (gz * per + within - row * per).astype(jnp.int32)
    row = row.astype(jnp.int32)
    at_lane = lax.broadcasted_iota(jnp.int32, (LANES, count), 0) == lane
    pmat[...] = jnp.where(at_lane, 1.0, 0.0).astype(pmat.dtype)
    at_row = lax.broadcasted_iota(jnp.int32, (PLANE, count), 0) == row
    own[...] = jnp.where(at_row, 1.0, 0.0)

    t = t_ref[...]
    pieces = jnp.concatenate(
        [own[...] * p.astype(jnp.float32) for p in (t & 255, (t >> 8) & 255, t >> 16)], axis=0
    ).astype(pmat.dtype)
    table = lax.dot_general(
        pieces, pmat[...], (((1,), (1,)), ((), ())), preferred_element_type=jnp.float32
    )
    tbuf[...] = (
        table[0:PLANE] + 256.0 * table[PLANE : 2 * PLANE] + 65536.0 * table[2 * PLANE :]
    ).astype(jnp.int32)

    def source_row(slot):
        kind, da, db = slot
        cs = c if kind == "o" else 1 - c
        xs = (x + da * (1 - cs) + db * cs) % NX
        ys = (y + da * cs + db * (1 - cs)) % NY
        return (xs * NY + ys) * 2 + cs

    rows = [source_row(slot) for slot in SLOTS]
    for k in range(PLANE):
        trel[:, k * block : (k + 1) * block] = tbuf[pl.ds(rows[k], 1), :][:, :block]

    pl.semaphore_wait(barrier, NZ - 1 + PLANE - 1)

    def along(o):
        return pltpu.make_async_remote_copy(
            src_ref=q_ref, dst_ref=zbuf.at[z], send_sem=zs_sem.at[o], recv_sem=zr_sem.at[z],
            device_id={"group": (z + o) % NZ}, device_id_type=MESH,
        )

    def along_in(o):
        other = (z + o) % NZ
        return pltpu.make_async_remote_copy(
            src_ref=q_ref, dst_ref=zbuf.at[other], send_sem=zs_sem.at[o], recv_sem=zr_sem.at[other],
            device_id={"group": other}, device_id_type=MESH,
        )

    for o in ALONG:
        along(o).start()
    zbuf[pl.ds(z, 1)] = q_ref[...][None]

    for o in ALONG:
        along_in(o).wait_recv()
    column = jnp.concatenate(
        [zbuf[k].astype(jnp.float32) for k in range(NZ)], axis=0
    ).astype(qall.dtype)
    for j in range(tiles):
        qall[0, j] = column[:, j * LANES : (j + 1) * LANES]

    sent = []

    def at(slot):
        return qall.at[PLACE[slot]]

    def copy(src, dst, device, sem):
        op = pltpu.make_async_remote_copy(
            src_ref=at(src), dst_ref=at(dst), send_sem=send_sem.at[len(sent)], recv_sem=sem,
            device_id=device, device_id_type=MESH,
        )
        op.start()
        sent.append(op)

    def over(src, ea, eb):
        _, da, db = src
        to = ("o", (da - ea) % 4, (db - eb) % 4)
        device = {
            "x": (x + ea * (1 - c) + eb * c) % NX,
            "y": (y + ea * c + eb * (1 - c)) % NY,
        }
        copy(src, to, device, own_sem.at[to[1] * 4 + to[2]])

    def across(src):
        _, da, db = src
        copy(src, ("m", da, db), {"core": 1 - c}, mate_sem.at[da * 4 + db])

    def arrived(slot):
        kind, da, db = slot
        sem = own_sem if kind == "o" else mate_sem
        pltpu.make_async_remote_copy(
            src_ref=at(slot), dst_ref=at(slot), send_sem=send_sem.at[0], recv_sem=sem.at[da * 4 + db],
            device_id={"core": 1 - c}, device_id_type=MESH,
        ).wait_recv()

    def passed_on(slot):
        kind, da, db = slot
        if kind == "m":
            return
        across(slot)
        if db == 0:
            over(slot, 0, 1)
            over(slot, 0, -1)
        if db == 1 and da in (2, 3):
            over(slot, 0, -1)
        if db == 3 and da in (0, 1):
            over(slot, 0, 1)

    mine = ("o", 0, 0)
    over(mine, 1, 0)
    over(mine, -1, 0)
    across(mine)
    arrived(("m", 0, 0))
    over(mine, 0, 1)
    over(mine, 0, -1)
    over(mine, 2, 0)

    def fresh():
        return (
            jnp.full((8, CHUNK), LOWEST, jnp.float32),
            jnp.zeros((8, CHUNK), jnp.float32),
            jnp.zeros((8, CHUNK), jnp.float32),
        )

    state = fresh()
    pending = None
    chunks = PLANE * block // CHUNK
    groups = block // 16

    def candidates_of(b):
        return jnp.concatenate(
            [cbuf[j, b * ROWS : (b + 1) * ROWS, :] for j in range(tiles)], axis=1
        )

    def queries_of(k):
        places = [divmod(k * CHUNK // 16 + i, groups) for i in range(CHUNK // 16)]
        return jnp.concatenate(
            [
                jnp.concatenate([qall[p, j, 16 * i : 16 * i + 16, :] for p, i in places], axis=0)
                for j in range(tiles)
            ],
            axis=1,
        )

    def drained(pending, state):
        k, b, side = pending
        mark = trel[:, k * CHUNK : (k + 1) * CHUNK] - base
        wanted = jnp.broadcast_to(mark >> 3, (8, CHUNK))
        state = folded(sbuf.at[side], ROWS // 8, *state, wanted, b * (ROWS // 8))
        if b < steps - 1:
            return state
        top, total, picked = state
        best = jnp.max(top, axis=0, keepdims=True)
        whole = jnp.sum(total * jnp.exp(top - best), axis=0, keepdims=True)
        line = lax.broadcasted_iota(jnp.int32, (8, CHUNK), 0)
        hit = jnp.where(line == (mark & 7), picked, 0.0)
        res[0:1, k * CHUNK : (k + 1) * CHUNK] = best + jnp.log(whole)
        res[1:2, k * CHUNK : (k + 1) * CHUNK] = jnp.sum(hit, axis=0, keepdims=True)
        return fresh()

    for load in loads:
        load.wait()
    for k in range(chunks):
        for b in range(steps):
            for slot in ARRIVALS.get((k, b), ()):
                arrived(slot)
                passed_on(slot)
            side = (k * steps + b) % 2
            sbuf[side] = lax.dot_general(
                candidates_of(b), queries_of(k),
                (((1,), (1,)), ((), ())), preferred_element_type=jnp.float32,
            )
            if pending is not None:
                state = drained(pending, state)
            pending = (k, b, side)
    drained(pending, state)

    for k in range(PLANE):
        part[rows[k], :, 0:block] = res[:, k * block : (k + 1) * block]

    def gathered(src, dst, s_sem, r_sem):
        ops = []
        for k, (dx, dy, dc) in enumerate(AROUND):
            device = {"x": (x + dx) % NX, "y": (y + dy) % NY, "core": (c + dc) % 2}
            other = (device["x"] * NY + device["y"]) * 2 + device["core"]
            op, back = (
                pltpu.make_async_remote_copy(
                    src_ref=src(other), dst_ref=dst.at[slot], send_sem=s_sem.at[k],
                    recv_sem=r_sem.at[slot], device_id=device, device_id_type=MESH,
                )
                for slot in (me, other)
            )
            op.start()
            ops.append((op, back))
        for _, back in ops:
            back.wait_recv()
        return ops

    inbox[pl.ds(me, 1)] = part[pl.ds(me, 1)]
    scattered = gathered(lambda other: part.at[other], inbox, rs_sem, rr_sem)
    lse, picked = merged(inbox[...])

    zin[pl.ds(z, 1), 0:1, :] = lse[None]
    zin[pl.ds(z, 1), 1:2, :] = picked[None]

    def reduce_to(o, at_me):
        other = (z + o) % NZ
        slot = z if at_me else other
        return pltpu.make_async_remote_copy(
            src_ref=zin.at[z], dst_ref=zin.at[slot], send_sem=gs_sem.at[o], recv_sem=gr_sem.at[slot],
            device_id={"group": other}, device_id_type=MESH,
        )

    for o in ALONG:
        reduce_to(o, True).start()
    for o in ALONG:
        reduce_to(o, False).wait_recv()
    lse, picked = merged(zin[...])

    outall[pl.ds(me, 1)] = (lse - picked)[None]
    spread = gathered(lambda other: outall.at[me], outall, as_sem, ar_sem)
    lanes = lax.broadcasted_iota(jnp.int32, (PLANE, LANES), 1)
    value = jnp.concatenate([outall[k] for k in range(PLANE)], axis=0)
    value = jnp.where(lanes < block, value, 0.0)
    high = value.astype(pmat.dtype)
    rest = value - high.astype(jnp.float32)
    middle = rest.astype(pmat.dtype)
    low = (rest - middle.astype(jnp.float32)).astype(pmat.dtype)
    spreads = jnp.dot(
        jnp.concatenate([high, middle, low], axis=0), pmat[...], preferred_element_type=jnp.float32
    )
    value = spreads[0:PLANE] + spreads[PLANE : 2 * PLANE] + spreads[2 * PLANE :]
    losses = jnp.sum(own[...] * value, axis=0, keepdims=True)
    out_ref[...] = losses
    mean_ref[0, 0] = jnp.sum(losses) / count

    for o in ALONG:
        along(o).wait_send()
        reduce_to(o, True).wait_send()
    for op in sent:
        op.wait_send()

    for op, _ in scattered + spread:
        op.wait_send()


def on_device(queries, candidates, targets):
    per, width = queries.shape
    block = NZ * per
    total = block * PLANE
    DMA = pltpu.SemaphoreType.DMA
    losses, mean = pl.pallas_call(
        kernel,
        out_shape=(
            jax.ShapeDtypeStruct((1, total), jnp.float32),
            jax.ShapeDtypeStruct((1, 1), jnp.float32),
        ),
        in_specs=[
            pl.BlockSpec(memory_space=pltpu.VMEM),
            pl.BlockSpec(memory_space=pltpu.VMEM),
            pl.BlockSpec(memory_space=pl.ANY),
        ],
        out_specs=(
            pl.BlockSpec(memory_space=pltpu.VMEM),
            pl.BlockSpec(memory_space=pltpu.SMEM),
        ),
        scratch_shapes=[
            pltpu.VMEM((NZ, per, width), jnp.bfloat16),
            pltpu.VMEM((PLANE, width // LANES, block, LANES), jnp.bfloat16),
            pltpu.VMEM((width // LANES, candidates.shape[0], LANES), jnp.bfloat16),
            pltpu.VMEM((2, ROWS, CHUNK), jnp.float32),
            pltpu.VMEM((LANES, total), jnp.bfloat16),
            pltpu.VMEM((PLANE, total), jnp.float32),
            pltpu.VMEM((PLANE, LANES), jnp.int32),
            pltpu.VMEM((1, total), jnp.int32),
            pltpu.VMEM((2, total), jnp.float32),
            pltpu.VMEM((PLANE, 2, LANES), jnp.float32),
            pltpu.VMEM((PLANE, 2, LANES), jnp.float32),
            pltpu.VMEM((NZ, 2, LANES), jnp.float32),
            pltpu.VMEM((PLANE, 1, LANES), jnp.float32),
            DMA((width // LANES,)),
            DMA((NZ,)),
            DMA((NZ,)),
            DMA((31,)),
            DMA((16,)),
            DMA((16,)),
            DMA((PLANE,)),
            DMA((PLANE,)),
            DMA((NZ,)),
            DMA((NZ,)),
            DMA((PLANE,)),
            DMA((PLANE,)),
        ],
        compiler_params=pltpu.CompilerParams(
            collective_id=0, has_side_effects=True, vmem_limit_bytes=56 * 2**20
        ),
    )(queries, targets.reshape(1, total), candidates)
    return losses.reshape(total), mean.reshape(())


def solution(mesh):
    finer = Mesh(mesh.devices.reshape(mesh.shape["group"], NX, NY, 2), EVERY)
    return jax.shard_map(
        on_device,
        mesh=finer,
        in_specs=(P(EVERY, None), P(EVERY, None), P()),
        out_specs=(P(), P()),
        check_vma=False,
    )
```
